32 devices in a mesh: row: 4 (over x, core), col: 8 (over z, y).
Axes of the slice: x: 2, y: 2, z: 4, core: 2. Of those that a mesh axis runs over, the one named last changes fastest.
Arguments:
- trailing: float32 [12288, 12288], P('row', 'col'), may hold values from -60 to 60
- near_panel: float32 [12288, 256], P('row', 'col'), may hold values from -0.0546875 to 0.0546875
- near_adjoint: float32 [12288, 256], P('row', 'col'), may hold values from -6 to 6
- near_block: float32 [256, 256], replicated, may hold values from -3 to 2, as said below
- near_inverse: float32 [256, 256], replicated, may hold values from -5 to 5, as said below
- near_block_adjoint: float32 [256, 256], replicated, may hold values from -6 to 6
- far_panel: float32 [12288, 256], P('row', 'col'), may hold values from -0.0546875 to 0.0546875
- far_adjoint: float32 [12288, 256], P('row', 'col'), may hold values from -6 to 6
- far_top: float32 [256, 256], replicated, may hold values from -0.375 to 0.375
- far_top_adjoint: float32 [256, 256], replicated, may hold values from -6 to 6
- far_block: float32 [256, 256], replicated, may hold values from -3 to 2, as said below
- far_inverse: float32 [256, 256], replicated, may hold values from -5 to 5, as said below
- far_block_adjoint: float32 [256, 256], replicated, may hold values from -6 to 6
Outputs:
- edge_adjoint: float32 [2, 12288, 256], P(None, 'row', 'col')
- corner_adjoint: float32 [512, 512], P('row', 'col')
The draws below stay inside these ranges and needn't reach their ends.
Inputs may be any that keep to these rules, and one draw needn't show every extreme that they name: `near_block`: lower triangular with diagonal entries of 1 to 2. `near_inverse`: the inverse of near_block, lower triangular. `far_block`: lower triangular with diagonal entries of 1 to 2. `far_inverse`: the inverse of far_block, lower triangular.
All inputs are finite; a program needn't handle non-finite values.
Results may differ from the reference program's by a relative error of at most 0.000098.
Values sent between devices are 32-bit elements; how exact they have to be, the bound alone decides.
A program may use at most 128 MiB of HBM per device.

```python
import jax
import jax.numpy as jnp
from jax import lax

M = 12288
B = 256


def lower_factor(key, salt):
    folded = jax.random.fold_in(key, salt)
    first, second = jax.random.split(folded)
    diagonal = jax.random.uniform(first, (B,), jnp.float32, 1.0, 2.0)
    spread = 0.5 * jax.random.normal(second, (B, B), jnp.float32) / B ** 0.5
    return jnp.tril(spread, -1) + jnp.diag(diagonal)


def lower_inverse(key, salt):
    factor = lower_factor(key, salt)
    return jnp.tril(jnp.linalg.inv(factor))


def draw_trailing(key, part):
    first = jax.random.fold_in(jax.random.fold_in(key, 3), 0)
    values = jax.random.normal(first, (M, M), jnp.float32)
    values = jnp.clip(values, -6.0, 6.0)
    return (values + values.T) * 0.7071


def draw_near_block(key, part):
    return lower_factor(key, 11)


def draw_near_inverse(key, part):
    return lower_inverse(key, 11)


def draw_far_block(key, part):
    return lower_factor(key, 29)


def draw_far_inverse(key, part):
    return lower_inverse(key, 29)


def block_levels(stream_key, shape, pieces, least, largest):
    factor_of = 1.0
    for dim, parts in pieces:
        heights = jax.random.uniform(jax.random.fold_in(jax.random.fold_in(stream_key, 6), dim), (parts,), jnp.float32, least / len(pieces), largest / len(pieces))
        factor_of = factor_of * jnp.repeat(jnp.exp(heights), shape[dim] // parts).reshape((-1,) + (1,) * (len(shape) - 1 - dim))
    return factor_of


def gaussian(rng, dims, scale, limit, shards=(), held_as=jnp.bfloat16):
    gain = block_levels(rng, dims, shards, -0.22, 0.18) if shards else 1.0
    drawn = jax.random.normal(rng, dims, jnp.float32) * scale * gain
    return jnp.minimum(jnp.maximum(drawn, -limit), limit).astype(held_as)


def setup_inputs(seed: int = 0) -> dict:
    arg_keys = jax.random.split(jax.random.key(seed), 14)
    trailing = draw_trailing(jax.random.fold_in(arg_keys[13], 71), 0)
    near_panel = gaussian(arg_keys[1], (M, B), M ** -0.5, 0.0546875, ((0, 4), (1, 8)), jnp.float32)
    near_adjoint = gaussian(arg_keys[2], (M, B), 1.0, 6.0, ((0, 4), (1, 8)), jnp.float32)
    near_block = draw_near_block(jax.random.fold_in(arg_keys[13], 71), 0)
    near_inverse = draw_near_inverse(jax.random.fold_in(arg_keys[13], 71), 0)
    near_block_adjoint = gaussian(arg_keys[5], (B, B), 1.0, 6.0, (), jnp.float32)
    far_panel = gaussian(arg_keys[6], (M, B), M ** -0.5, 0.0546875, ((0, 4), (1, 8)), jnp.float32)
    far_adjoint = gaussian(arg_keys[7], (M, B), 1.0, 6.0, ((0, 4), (1, 8)), jnp.float32)
    far_top = gaussian(arg_keys[8], (B, B), B ** -0.5, 0.375, (), jnp.float32)
    far_top_adjoint = gaussian(arg_keys[9], (B, B), 1.0, 6.0, (), jnp.float32)
    far_block = draw_far_block(jax.random.fold_in(arg_keys[13], 71), 0)
    far_inverse = draw_far_inverse(jax.random.fold_in(arg_keys[13], 71), 0)
    far_block_adjoint = gaussian(arg_keys[12], (B, B), 1.0, 6.0, (), jnp.float32)
    return dict(trailing=trailing, near_panel=near_panel, near_adjoint=near_adjoint, near_block=near_block, near_inverse=near_inverse, near_block_adjoint=near_block_adjoint, far_panel=far_panel, far_adjoint=far_adjoint, far_top=far_top, far_top_adjoint=far_top_adjoint, far_block=far_block, far_inverse=far_inverse, far_block_adjoint=far_block_adjoint)


def multiply(left, right):
    return jnp.dot(left.astype(jnp.float32), right.astype(jnp.float32), precision=lax.Precision.HIGHEST, preferred_element_type=jnp.float32)

def block_reverse(factor, inverse, adjoint):
    product = multiply(factor.T, adjoint)
    halved = jnp.tril(product) - 0.5 * jnp.diag(jnp.diag(product))
    middle = multiply(multiply(inverse.T, halved), inverse)
    return 0.5 * (middle + middle.T)

def reference(trailing, near_panel, near_adjoint, near_block, near_inverse, near_block_adjoint, far_panel, far_adjoint, far_top, far_top_adjoint, far_block, far_inverse, far_block_adjoint):
    near_grad = near_adjoint - 2.0 * multiply(trailing, near_panel)
    near_result = multiply(near_grad, near_inverse)
    near_corner = block_reverse(near_block, near_inverse, near_block_adjoint - multiply(near_result.T, near_panel))
    top_grad = far_top_adjoint - 2.0 * multiply(near_corner, far_top) - multiply(near_result.T, far_panel)
    top_result = multiply(top_grad, far_inverse)
    far_grad = far_adjoint - multiply(near_result, far_top) - 2.0 * multiply(trailing, far_panel)
    far_result = multiply(far_grad, far_inverse)
    far_corner = block_reverse(far_block, far_inverse, far_block_adjoint - multiply(top_result.T, far_top) - multiply(far_result.T, far_panel))
    edge_adjoint = jnp.stack([0.5 * far_result, 0.5 * near_result])
    upper = jnp.concatenate([far_corner, 0.5 * top_result.T], axis=1)
    lower = jnp.concatenate([0.5 * top_result, near_corner], axis=1)
    corner_adjoint = jnp.concatenate([upper, lower], axis=0)
    return (edge_adjoint, corner_adjoint)
```

```python
import jax
import jax.numpy as jnp
from jax import lax
from jax.sharding import PartitionSpec as P


PRECISION = lax.Precision.HIGH


def contract(left, right, left_dim, right_dim):
    return lax.dot_general(
        left,
        right,
        (((left_dim,), (right_dim,)), ((), ())),
        precision=PRECISION,
        preferred_element_type=jnp.float32,
    )


def multiply(left, right):
    return contract(left, right, 1, 0)


def block_reverse(factor, inverse, adjoint):
    product = contract(factor, adjoint, 0, 0)
    size = product.shape[0]
    rows = lax.broadcasted_iota(jnp.int32, (size, size), 0)
    cols = lax.broadcasted_iota(jnp.int32, (size, size), 1)
    weight = jnp.where(rows > cols, 1.0, jnp.where(rows == cols, 0.5, 0.0))
    halved = jnp.where(rows >= cols, product * weight, 0.0)
    middle = multiply(contract(inverse, halved, 0, 0), inverse)
    return 0.5 * (middle + middle.T)


def to_slabs(shards):
    cols = lax.axis_size("col")
    count = len(shards)
    rows, width = shards[0].shape
    turned = jnp.stack([shard.T for shard in shards])
    pieces = turned.reshape(count, width, cols, rows // cols).transpose(2, 0, 1, 3)
    moved = lax.all_to_all(pieces, "col", 0, 0)
    return moved.transpose(1, 0, 2, 3).reshape(count, cols * width, rows // cols)


def from_slabs(slabs):
    cols = lax.axis_size("col")
    count, columns, slab = slabs.shape
    width = columns // cols
    pieces = slabs.reshape(count, cols, width, slab).transpose(1, 0, 2, 3)
    moved = lax.all_to_all(pieces, "col", 0, 0)
    return moved.transpose(1, 0, 3, 2).reshape(count, cols * slab, width)


def flip(block, axis, bit):
    pairs = [(index, index ^ bit) for index in range(lax.axis_size(axis))]
    return lax.ppermute(block, axis, pairs)


def bits_of(axis):
    bits = []
    bit = lax.axis_size(axis) // 2
    while bit:
        bits.append(bit)
        bit //= 2
    return bits


def beside_slabs(slabs):
    rows, cols = lax.axis_size("row"), lax.axis_size("col")
    ratio = cols // rows
    pairs = []
    for col in range(cols):
        for row in range(rows):
            source = (col // ratio) * cols + (col % ratio) * rows + row
            pairs.append((source, row * cols + col))
    held = lax.ppermute(slabs, ("row", "col"), pairs)[None]
    row_index = lax.axis_index("row")
    bits = bits_of("row")
    for bit in bits:
        other = flip(held, "row", bit)
        upper = (row_index & bit) != 0
        held = jnp.concatenate(
            [jnp.where(upper, other, held), jnp.where(upper, held, other)], axis=0
        )
    held = held.reshape((2,) * len(bits) + slabs.shape)
    order = tuple(reversed(range(len(bits))))
    count = len(bits)
    held = held.transpose(order + tuple(range(count, count + 3)))
    held = held.reshape((rows,) + slabs.shape).transpose(1, 2, 0, 3)
    return held.reshape(slabs.shape[0], slabs.shape[1], rows * slabs.shape[2])


def ring_place(col):
    cols = lax.axis_size("col")
    return jnp.where(col % 2 == 0, col // 2, cols - 1 - col // 2)


def ring_column(place):
    cols = lax.axis_size("col")
    return jnp.where(place < cols // 2, 2 * place, 2 * (cols - 1 - place) + 1)


def ring_sums(trailing, besides, adjoints):
    cols = lax.axis_size("col")
    col_index = lax.axis_index("col")
    place = ring_place(col_index)
    order = list(range(0, cols, 2)) + list(range(cols - 1, 0, -2))
    slab = trailing.shape[0] // cols
    placed = []
    for adjoint in adjoints:
        width = adjoint.shape[1]
        empty = jnp.zeros((cols * width, adjoint.shape[0]), adjoint.dtype)
        placed.append(lax.dynamic_update_slice_in_dim(empty, adjoint.T, col_index * width, 0))

    def term(index, start):
        rows = lax.dynamic_slice_in_dim(trailing, start, slab, 0)
        added = lax.dynamic_slice_in_dim(placed[index], start, slab, 1)
        return added - 2.0 * contract(besides[index], rows, 1, 1)

    running = [None, None]
    for step in range(cols):
        for index, way in enumerate((1, -1)):
            target = (place - way * (1 + step)) % cols
            here = term(index, ring_column(target) * slab)
            running[index] = here if step == 0 else running[index] + here
        if step < cols - 1:
            for index, way in enumerate((1, -1)):
                pairs = [(order[i], order[(i + way) % cols]) for i in range(cols)]
                running[index] = lax.ppermute(running[index], "col", pairs)
    return running


def total_everywhere(block):
    steps = [(axis, bit) for axis in ("row", "col") for bit in reversed(bits_of(axis))]
    for axis, bit in steps:
        upper = (lax.axis_index(axis) & bit) != 0
        half = block.shape[1] // 2
        low, high = block[:, :half], block[:, half:]
        kept, sent = jnp.where(upper, high, low), jnp.where(upper, low, high)
        block = kept + flip(sent, axis, bit)
    for axis, bit in reversed(steps):
        upper = (lax.axis_index(axis) & bit) != 0
        other = flip(block, axis, bit)
        block = jnp.concatenate(
            [jnp.where(upper, other, block), jnp.where(upper, block, other)], axis=1
        )
    return block


def per_device(
    trailing,
    near_panel,
    near_adjoint,
    near_block,
    near_inverse,
    near_block_adjoint,
    far_panel,
    far_adjoint,
    far_top,
    far_top_adjoint,
    far_block,
    far_inverse,
    far_block_adjoint,
):
    row_index = lax.axis_index("row")
    col_index = lax.axis_index("col")
    panels = [to_slabs([near_panel]), to_slabs([far_panel])]
    near_rows, far_rows = panels[0][0], panels[1][0]
    beside = [beside_slabs(panel)[0] for panel in panels]
    size = near_block.shape[0]
    near_grad, far_grad = ring_sums(trailing, beside, [near_adjoint, far_adjoint])
    near_result = contract(near_inverse, near_grad, 0, 0)
    far_grad = far_grad - contract(far_top, near_result, 0, 0)
    far_result = contract(far_inverse, far_grad, 0, 0)
    parts = [
        contract(near_result, near_rows, 1, 1),
        contract(near_result, far_rows, 1, 1),
        contract(far_result, far_rows, 1, 1),
    ]
    fold = lax.axis_size("row") * lax.axis_size("col")
    joined = jnp.concatenate(parts, axis=0)
    depth = 8 * fold if joined.size % (8 * fold * 128) == 0 else fold
    totals = total_everywhere(joined.reshape(-1, depth, 128))
    totals = totals.reshape(3, size, size)
    near_totals = jnp.concatenate([totals[0], totals[1]], axis=1)
    far_totals = totals[2]
    edge_out = from_slabs(0.5 * jnp.stack([far_result, near_result]))

    near_corner = block_reverse(
        near_block, near_inverse, near_block_adjoint - near_totals[:, :size]
    )
    top_grad = far_top_adjoint - 2.0 * multiply(near_corner, far_top) - near_totals[:, size:]
    top_result = multiply(top_grad, far_inverse)
    far_corner = block_reverse(
        far_block, far_inverse, far_block_adjoint - contract(top_result, far_top, 0, 0) - far_totals
    )
    upper = jnp.concatenate([far_corner, 0.5 * top_result.T], axis=1)
    lower = jnp.concatenate([0.5 * top_result, near_corner], axis=1)
    corner = jnp.concatenate([upper, lower], axis=0)
    corner_rows = corner.shape[0] // lax.axis_size("row")
    corner_cols = corner.shape[1] // lax.axis_size("col")
    corner_out = lax.dynamic_slice(
        corner, (row_index * corner_rows, col_index * corner_cols), (corner_rows, corner_cols)
    )
    return (edge_out, corner_out)


def solution(mesh):
    in_specs = (
        P("row", "col"),
        P("row", "col"),
        P("row", "col"),
        P(),
        P(),
        P(),
        P("row", "col"),
        P("row", "col"),
        P(),
        P(),
        P(),
        P(),
        P(),
    )
    out_specs = (P(None, "row", "col"), P("row", "col"))
    return jax.shard_map(
        per_device, mesh=mesh, in_specs=in_specs, out_specs=out_specs, check_vma=False
    )
```
